8 devices in a mesh: dp: 1 (over z), cy: 2 (over y), cx: 4 (over x, core).
Axes of the slice: x: 2, y: 2, z: 1, core: 2. Of those that a mesh axis runs over, the one named last changes fastest.
Arguments:
- queries: bfloat16 [16384, 32, 128], P(('dp', 'cx', 'cy'))
- keys: bfloat16 [16384, 8, 128], P(('dp', 'cx', 'cy'))
- values: bfloat16 [16384, 8, 128], P(('dp', 'cx', 'cy'))
- doc_ids: int32 [16384], P(('dp', 'cx', 'cy'))
Outputs:
- output: bfloat16 [16384, 32, 128], P(('dp', 'cx', 'cy'))
All inputs are finite; a program needn't handle non-finite values.
Results may differ from the reference program's by a relative error of at most 0.0012794.
Values are sent between devices in bfloat16 or wider.
A program may use at most 1 GiB of HBM per device.

```python
import jax
import jax.numpy as jnp
from jax import lax

SEQ_LEN = 16384
GROUP_SIZE = 8
HEADS = 32
KV_HEADS = 8
HEAD_DIM = 128
DOC_COUNT = 6
ROW_BLOCK = 16

TOKENS_DEV = SEQ_LEN // GROUP_SIZE
PIECE_LEN = TOKENS_DEV // 2
Q_PER_KV = HEADS // KV_HEADS


def layout_positions():
    row_ids = jnp.arange(SEQ_LEN)
    dev_rank = row_ids // TOKENS_DEV
    in_dev = row_ids % TOKENS_DEV
    piece_ids = jnp.where(in_dev < PIECE_LEN, dev_rank, 2 * GROUP_SIZE - 1 - dev_rank)
    return piece_ids * PIECE_LEN + in_dev % PIECE_LEN


def draw_segments(seg_key):
    cut_points = jax.random.permutation(seg_key, SEQ_LEN - 1)[:DOC_COUNT - 1] + 1
    return jnp.sum(layout_positions()[:, None] >= cut_points[None, :], axis=1).astype(jnp.int32)


def setup_inputs(seed: int = 0, part: int = 0) -> dict:
    part_key = jax.random.fold_in(jax.random.key(seed), part)
    key_q, key_k, key_v, key_shift, key_seg = jax.random.split(part_key, 5)
    q_arr = jax.random.normal(key_q, (SEQ_LEN, HEADS, HEAD_DIM), jnp.float32)
    k_arr = jax.random.normal(key_k, (SEQ_LEN, KV_HEADS, HEAD_DIM), jnp.float32)
    v_noise = jax.random.normal(key_v, (2 * GROUP_SIZE, PIECE_LEN, KV_HEADS, HEAD_DIM), jnp.float32)
    v_shift = jax.random.normal(key_shift, (2 * GROUP_SIZE, 1, KV_HEADS, HEAD_DIM), jnp.float32)
    v_arr = (v_noise + v_shift).reshape(SEQ_LEN, KV_HEADS, HEAD_DIM)
    return {'queries': q_arr.astype(jnp.bfloat16), 'keys': k_arr.astype(jnp.bfloat16), 'values': v_arr.astype(jnp.bfloat16), 'doc_ids': draw_segments(key_seg)}


def reference(queries, keys, values, doc_ids):
    positions = layout_positions()
    score_scale = HEAD_DIM ** -0.5
    keys_f32 = keys.astype(jnp.float32)
    vals_f32 = values.astype(jnp.float32)
    q_blocks = queries.reshape(SEQ_LEN // ROW_BLOCK, ROW_BLOCK, KV_HEADS, Q_PER_KV, HEAD_DIM)
    pos_blocks = positions.reshape(SEQ_LEN // ROW_BLOCK, ROW_BLOCK)
    doc_blocks = doc_ids.reshape(SEQ_LEN // ROW_BLOCK, ROW_BLOCK)

    def one_block(block_in):
        q_blk, q_pos, q_doc = block_in
        scores = jnp.einsum('qgjd,kgd->qgjk', q_blk.astype(jnp.float32), keys_f32) * score_scale
        allowed = (positions[None, :] <= q_pos[:, None]) & (doc_ids[None, :] == q_doc[:, None])
        key_mask = allowed[:, None, None, :]
        row_max = jnp.max(jnp.where(key_mask, scores, -1e30), axis=-1, keepdims=True)
        weights = jnp.exp(jnp.where(key_mask, scores - row_max, -1e30))
        denominator = jnp.sum(weights, axis=-1)
        numerator = jnp.einsum('qgjk,kgd->qgjd', weights.astype(jnp.bfloat16).astype(jnp.float32), vals_f32)
        return (numerator / denominator[..., None]).astype(jnp.bfloat16)

    out_blocks = lax.map(one_block, (q_blocks, pos_blocks, doc_blocks))
    return out_blocks.reshape(SEQ_LEN, HEADS, HEAD_DIM)
```

```python
import functools
import math

import jax
import jax.numpy as jnp
from jax import lax
from jax.experimental import pallas as pl
from jax.experimental.pallas import tpu as pltpu
from jax.sharding import PartitionSpec as P

DOCS = 6
BLK = 256
CHUNKS = (2, 2, 2, 2)
HEAD_DIM = 128
SCALE_LOG2 = HEAD_DIM ** -0.5 * math.log2(math.e)
NEG_BIG = -1e30 * HEAD_DIM ** 0.5


def attend_kernel(tab_ref, rng_ref, kv_hbm, qt_ref, start_ref, out_ref, kv_scr, s_scr, p_scr, acc_scr, max_scr, sum_scr, fac_scr, sems, *, heads, head_lo, pieces, piece_len, q_per_kv):
    head = pl.program_id(0)
    tile = pl.program_id(1)
    tiles_piece = piece_len // BLK
    slot = lax.rem(head, 2)

    def piece_copy(head_idx, slot_idx, piece):
        upper = piece >= pieces // 2
        rank = jnp.where(upper, pieces - 1 - piece, piece)
        row = jnp.where(upper, piece_len, 0)
        return pltpu.make_async_copy(
            kv_hbm.at[rank, :, head_idx, pl.ds(pl.multiple_of(row, piece_len), piece_len), :],
            kv_scr.at[slot_idx, :, pl.ds(pl.multiple_of(piece * piece_len, piece_len), piece_len), :],
            sems.at[slot_idx, piece])

    def over_range(which, fn):
        def body(piece, _):
            fn(piece)
            return 0
        lax.fori_loop(rng_ref[which, 0], rng_ref[which, 1], body, 0)

    def start_head(head_idx):
        slot_idx = lax.rem(head_idx, 2)
        for which in range(2):
            over_range(which, lambda piece: piece_copy(head_idx, slot_idx, piece).start())

    @pl.when((head == 0) & (tile == 0))
    def _():
        start_head(head)

    @pl.when(tile == 0)
    def _():
        @pl.when(head + 1 < heads)
        def _():
            start_head(head + 1)
        over_range(0, lambda piece: piece_copy(head, slot, piece).wait())

    @pl.when(tile == tiles_piece)
    def _():
        over_range(1, lambda piece: piece_copy(head, slot, piece).wait())

    blk_lo = tab_ref[0, tile]
    blk_hi = tab_ref[1, tile]
    start_last = tab_ref[2, tile]

    def cols(col):
        return pl.ds(col * BLK, BLK)

    def rows(blk):
        return pl.ds(pl.multiple_of(blk * BLK, BLK), BLK)

    def score(k_blk, col):
        s_scr[:, cols(col)] = jnp.dot(k_blk, qt_ref[0, 0, :, cols(col)], preferred_element_type=jnp.float32)

    def load_v(blk):
        v_blk = kv_scr[slot, 1, rows(blk), :]
        return jnp.concatenate([v_blk[i * HEAD_DIM:(i + 1) * HEAD_DIM] for i in range(BLK // HEAD_DIM)], axis=1)

    def product(v_blk, col):
        acc_scr[:, cols(col)] = acc_scr[:, cols(col)] * fac_scr[:, cols(col)] + jnp.dot(v_blk, p_scr[:, cols(col)], preferred_element_type=jnp.float32)

    def soften(col):
        scores = s_scr[:, cols(col)]
        max_old = max_scr[:, cols(col)]
        max_new = jnp.maximum(max_old, jnp.max(scores, axis=0, keepdims=True))
        weights = jnp.exp2((scores - max_new) * SCALE_LOG2)
        fac = jnp.exp2((max_old - max_new) * SCALE_LOG2)
        sum_scr[:, cols(col)] = sum_scr[:, cols(col)] * fac + jnp.sum(weights, axis=0, keepdims=True)
        max_scr[:, cols(col)] = max_new
        fac_scr[:, cols(col)] = fac
        p_scr[:, cols(col)] = weights.astype(jnp.bfloat16)

    p_scr[...] = jnp.zeros_like(p_scr)
    acc_scr[...] = jnp.zeros_like(acc_scr)
    fac_scr[...] = jnp.zeros_like(fac_scr)
    sum_scr[...] = jnp.zeros_like(sum_scr)
    max_scr[...] = jnp.full_like(max_scr, NEG_BIG)
    k_first = kv_scr[slot, 0, rows(blk_lo), :]
    for col in range(q_per_kv):
        score(k_first, col)

    def step(blk, _):
        @pl.when((blk == blk_hi) | (blk * BLK < start_last))
        def _():
            k_pos = blk * BLK + lax.broadcasted_iota(jnp.int32, (BLK, BLK), 0)
            q_pos = blk_hi * BLK + lax.broadcasted_iota(jnp.int32, (BLK, BLK), 1)
            allowed = (k_pos <= q_pos) & (k_pos >= start_ref[0])
            for col in range(q_per_kv):
                s_scr[:, cols(col)] = jnp.where(allowed, s_scr[:, cols(col)], NEG_BIG)

        v_prev = load_v(jnp.maximum(blk - 1, blk_lo))
        k_next = kv_scr[slot, 0, rows(jnp.minimum(blk + 1, blk_hi)), :]
        for col in range(q_per_kv):
            product(v_prev, col)
            soften(col)
            score(k_next, col)
        return 0

    lax.fori_loop(blk_lo, blk_hi + 1, step, 0)
    v_last = load_v(blk_hi)
    for col in range(q_per_kv):
        product(v_last, col)
        normed = acc_scr[:, cols(col)] * (1.0 / sum_scr[:, cols(col)])
        out_ref[col] = normed.T.astype(jnp.bfloat16)


def attend(tab, rng, kv_all, qt_all, starts, head_lo, heads):
    ranks, _, _, tok_dev, head_dim = kv_all.shape
    pieces = 2 * ranks
    piece_len = tok_dev // 2
    tiles = tok_dev // BLK
    wide = qt_all.shape[-1]
    q_per_kv = wide // BLK
    body = functools.partial(attend_kernel, heads=heads, head_lo=head_lo, pieces=pieces, piece_len=piece_len, q_per_kv=q_per_kv)
    pairs = ranks * tok_dev * tok_dev // 4
    return pl.pallas_call(
        body,
        grid_spec=pltpu.PrefetchScalarGridSpec(
            num_scalar_prefetch=2,
            grid=(heads, tiles),
            in_specs=[
                pl.BlockSpec(memory_space=pl.ANY),
                pl.BlockSpec((1, 1, head_dim, wide), lambda h, t, *_: (h + head_lo, t, 0, 0)),
                pl.BlockSpec((1, 1, BLK), lambda h, t, *_: (t, 0, 0)),
            ],
            out_specs=pl.BlockSpec((q_per_kv, BLK, head_dim), lambda h, t, *_: (h, t, 0)),
            scratch_shapes=[
                pltpu.VMEM((2, 2, pieces * piece_len, head_dim), jnp.bfloat16),
                pltpu.VMEM((BLK, wide), jnp.float32),
                pltpu.VMEM((BLK, wide), jnp.bfloat16),
                pltpu.VMEM((head_dim, wide), jnp.float32),
                pltpu.VMEM((1, wide), jnp.float32),
                pltpu.VMEM((1, wide), jnp.float32),
                pltpu.VMEM((1, wide), jnp.float32),
                pltpu.SemaphoreType.DMA((2, pieces)),
            ],
        ),
        out_shape=jax.ShapeDtypeStruct((heads * q_per_kv, tok_dev, head_dim), jnp.bfloat16),
        compiler_params=pltpu.CompilerParams(dimension_semantics=("arbitrary", "arbitrary"), vmem_limit_bytes=48 * 1024 * 1024),
        cost_estimate=pl.CostEstimate(flops=pairs * heads * q_per_kv * 4 * head_dim, bytes_accessed=heads * pieces * piece_len * head_dim * 4, transcendentals=pairs * heads * q_per_kv),
    )(tab, rng, kv_all, qt_all, starts)


def solution(mesh):
    size_cy = mesh.shape['cy']
    group = mesh.shape['cx'] * size_cy
    seq_spec = P(('dp', 'cx', 'cy'), None, None)
    doc_spec = P(('dp', 'cx', 'cy'))

    def per_device(q_loc, k_loc, v_loc, doc_loc):
        tok_dev, num_heads, head_dim = q_loc.shape
        kv_heads = k_loc.shape[1]
        q_per_kv = num_heads // kv_heads
        piece_len = tok_dev // 2
        tiles = tok_dev // BLK
        rank = lax.axis_index('cx') * size_cy + lax.axis_index('cy')

        k_heads = k_loc.transpose(1, 0, 2)
        v_heads = v_loc.reshape(tok_dev // head_dim, head_dim, kv_heads, head_dim).transpose(2, 0, 3, 1).reshape(kv_heads, tok_dev, head_dim)
        gathered = []
        head_lo = 0
        for heads in CHUNKS:
            part = jnp.stack([k_heads[head_lo:head_lo + heads], v_heads[head_lo:head_lo + heads]])
            gathered.append(lax.all_gather(part, ('cx', 'cy')))
            head_lo += heads

        below = jnp.sum(doc_loc[None, :] < jnp.arange(DOCS, dtype=jnp.int32)[:, None], axis=1, dtype=jnp.int32)
        below = lax.psum(below, ('cx', 'cy'))
        starts = jnp.zeros_like(doc_loc)
        for doc in range(DOCS):
            starts = jnp.where(doc_loc == doc, below[doc], starts)
        starts = starts.reshape(tiles, 1, BLK)
        tile_ids = jnp.arange(tiles, dtype=jnp.int32)
        half = tiles // 2
        tile_blk = jnp.where(tile_ids < half, rank * half + tile_ids, (2 * group - 1 - rank) * half + tile_ids - half).astype(jnp.int32)
        tab = jnp.stack([starts[:, 0, 0] // BLK, tile_blk, starts[:, 0, BLK - 1]])
        first_lo = starts[0, 0, 0] // piece_len
        second_lo = starts[half, 0, 0] // piece_len
        first_end = rank + 1
        rng = jnp.stack([jnp.stack([jnp.minimum(first_lo, second_lo), first_end]), jnp.stack([jnp.maximum(second_lo, first_end), 2 * group - rank])]).astype(jnp.int32)

        qt = q_loc.reshape(tiles, BLK, kv_heads, q_per_kv, head_dim).transpose(2, 0, 4, 3, 1).reshape(kv_heads, tiles, head_dim, q_per_kv * BLK)
        outs = []
        head_lo = 0
        for heads, kv_all in zip(CHUNKS, gathered):
            outs.append(attend(tab, rng, kv_all, qt, starts, head_lo, heads))
            head_lo += heads
        return jnp.concatenate(outs, axis=0).transpose(1, 0, 2)

    return jax.shard_map(per_device, mesh=mesh, in_specs=(seq_spec, seq_spec, seq_spec, doc_spec), out_specs=seq_spec, check_vma=False)
```

```python
import functools
import math

import jax
import jax.numpy as jnp
from jax import lax
from jax.experimental import pallas as pl
from jax.experimental.pallas import tpu as pltpu
from jax.sharding import PartitionSpec as P

DOCS = 6
TILE = 256
BLK = 256
LANES = 128
CHUNK = 2
HEAD_DIM = 128
KV_HEADS = 8
SCALE_LOG2 = HEAD_DIM ** -0.5 * math.log2(math.e)
NEG_BIG = -1e30 * HEAD_DIM ** 0.5


def attend_kernel(tab_ref, rng_ref, kv_hbm, q_ref, start_ref, *rest, heads, pieces, piece_len, q_per_kv):
    out_ref, kv_scr, q_scr, qt_scr, s_scr, p_scr, acc_scr, top_scr, max_scr, sum_scr, fac_scr, sems = rest[-12:]
    tile = pl.program_id(0)
    tiles_piece = piece_len // TILE
    q_heads = heads * q_per_kv
    halves = TILE // LANES

    def piece_copy(piece):
        upper = piece >= pieces // 2
        rank = jnp.where(upper, pieces - 1 - piece, piece)
        row = jnp.where(upper, piece_len, 0)
        return pltpu.make_async_copy(
            kv_hbm.at[rank, :, :, pl.ds(pl.multiple_of(row, piece_len), piece_len), :],
            kv_scr.at[:, :, pl.ds(pl.multiple_of(piece * piece_len, piece_len), piece_len), :],
            sems.at[piece])

    def over_range(which, fn):
        def body(piece, _):
            fn(piece)
            return 0
        lax.fori_loop(rng_ref[which, 0], rng_ref[which, 1], body, 0)

    @pl.when(tile == 0)
    def _():
        over_range(0, lambda piece: piece_copy(piece).start())
        over_range(1, lambda piece: piece_copy(piece).start())

    q_scr[...] = q_ref[...].astype(jnp.float32).reshape(TILE * q_heads, HEAD_DIM)
    for head in range(q_heads):
        q_head = q_scr[pl.ds(head, TILE, stride=q_heads), :].T.astype(jnp.bfloat16)
        for half in range(halves):
            qt_scr[head * halves + half] = q_head[:, half * LANES:(half + 1) * LANES]

    @pl.when(tile == 0)
    def _():
        over_range(0, lambda piece: piece_copy(piece).wait())

    @pl.when(tile == tiles_piece)
    def _():
        over_range(1, lambda piece: piece_copy(piece).wait())

    blk_lo = tab_ref[0, tile]
    blk_hi = tab_ref[1, tile]
    start_last = tab_ref[2, tile]

    def cols(head):
        return pl.ds(head * TILE, TILE)

    def rows(blk):
        return pl.ds(pl.multiple_of(blk * BLK, BLK), BLK)

    def score(k_blk, head):
        q_head = jnp.concatenate([qt_scr[head * halves + half] for half in range(halves)], axis=1)
        scores = jnp.dot(k_blk, q_head, preferred_element_type=jnp.float32)
        s_scr[:, cols(head)] = scores
        top_scr[:, cols(head)] = jnp.max(scores, axis=0, keepdims=True)

    def load_v(kv_head, blk):
        v_blk = kv_scr[1, kv_head, rows(blk), :]
        return jnp.concatenate([v_blk[i * HEAD_DIM:(i + 1) * HEAD_DIM] for i in range(BLK // HEAD_DIM)], axis=1)

    def product(v_blk, head):
        p_head = jnp.concatenate([p_scr[head * halves + half] for half in range(halves)], axis=1)
        acc_scr[:, cols(head)] = acc_scr[:, cols(head)] * fac_scr[:, cols(head)] + jnp.dot(v_blk, p_head, preferred_element_type=jnp.float32)

    def soften(head):
        max_old = max_scr[:, cols(head)]
        max_new = jnp.maximum(max_old, top_scr[:, cols(head)])
        fac = jnp.exp2((max_old - max_new) * SCALE_LOG2)
        max_scr[:, cols(head)] = max_new
        fac_scr[:, cols(head)] = fac
        weights = jnp.exp2((s_scr[:, cols(head)] - max_new) * SCALE_LOG2)
        sum_scr[:, cols(head)] = sum_scr[:, cols(head)] * fac + jnp.sum(weights, axis=0, keepdims=True)
        for half in range(halves):
            p_scr[head * halves + half] = weights[:, half * LANES:(half + 1) * LANES].astype(jnp.bfloat16)

    p_scr[...] = jnp.zeros_like(p_scr)
    acc_scr[...] = jnp.zeros_like(acc_scr)
    fac_scr[...] = jnp.zeros_like(fac_scr)
    sum_scr[...] = jnp.zeros_like(sum_scr)
    max_scr[...] = jnp.full_like(max_scr, NEG_BIG)
    for kv_head in range(heads):
        k_first = kv_scr[0, kv_head, rows(blk_lo), :]
        for col in range(q_per_kv):
            score(k_first, kv_head * q_per_kv + col)

    def step(blk, _):
        @pl.when((blk == blk_hi) | (blk * BLK < start_last))
        def _():
            k_pos = blk * BLK + lax.broadcasted_iota(jnp.int32, (BLK, TILE), 0)
            q_pos = blk_hi * TILE + lax.broadcasted_iota(jnp.int32, (BLK, TILE), 1)
            allowed = (k_pos <= q_pos) & (k_pos >= start_ref[0])
            for head in range(q_heads):
                scores = jnp.where(allowed, s_scr[:, cols(head)], NEG_BIG)
                s_scr[:, cols(head)] = scores
                top_scr[:, cols(head)] = jnp.max(scores, axis=0, keepdims=True)

        for kv_head in range(heads):
            v_prev = load_v(kv_head, jnp.maximum(blk - 1, blk_lo))
            k_next = kv_scr[0, kv_head, rows(jnp.minimum(blk + 1, blk_hi)), :]
            for col in range(q_per_kv):
                head = kv_head * q_per_kv + col
                product(v_prev, head)
                soften(head)
                score(k_next, head)
        return 0

    lax.fori_loop(blk_lo, blk_hi + 1, step, 0)
    for kv_head in range(heads):
        v_last = load_v(kv_head, blk_hi)
        for col in range(q_per_kv):
            head = kv_head * q_per_kv + col
            product(v_last, head)
            normed = acc_scr[:, cols(head)] * (1.0 / sum_scr[:, cols(head)])
            q_scr[pl.ds(head, TILE, stride=q_heads), :] = normed.T
    out_ref[...] = q_scr[...].reshape(TILE, q_heads, HEAD_DIM).astype(jnp.bfloat16)


def attend(tab, rng, kv_all, q_loc, starts, prev, chunk):
    ranks, _, heads, tok_dev, head_dim = kv_all.shape
    num_heads = q_loc.shape[1]
    pieces = 2 * ranks
    piece_len = tok_dev // 2
    tiles = tok_dev // TILE
    q_per_kv = num_heads // KV_HEADS
    q_heads = heads * q_per_kv
    wide = q_heads * TILE
    body = functools.partial(attend_kernel, heads=heads, pieces=pieces, piece_len=piece_len, q_per_kv=q_per_kv)
    pairs = ranks * tok_dev * tok_dev // 4
    operands = [tab, rng, kv_all, q_loc, starts]
    in_specs = [
        pl.BlockSpec(memory_space=pl.ANY),
        pl.BlockSpec((TILE, q_heads, head_dim), lambda t, *_: (t, chunk, 0)),
        pl.BlockSpec((1, 1, TILE), lambda t, *_: (t, 0, 0)),
    ]
    aliases = {}
    if prev is not None:
        operands.append(prev)
        in_specs.append(pl.BlockSpec(memory_space=pl.ANY))
        aliases = {5: 0}
    return pl.pallas_call(
        body,
        grid_spec=pltpu.PrefetchScalarGridSpec(
            num_scalar_prefetch=2,
            grid=(tiles,),
            in_specs=in_specs,
            out_specs=pl.BlockSpec((TILE, q_heads, head_dim), lambda t, *_: (t, chunk, 0)),
            scratch_shapes=[
                pltpu.VMEM((2, heads, pieces * piece_len, head_dim), jnp.bfloat16),
                pltpu.VMEM((TILE * q_heads, head_dim), jnp.float32),
                pltpu.VMEM((wide // LANES, head_dim, LANES), jnp.bfloat16),
                pltpu.VMEM((BLK, wide), jnp.float32),
                pltpu.VMEM((wide // LANES, BLK, LANES), jnp.bfloat16),
                pltpu.VMEM((head_dim, wide), jnp.float32),
                pltpu.VMEM((1, wide), jnp.float32),
                pltpu.VMEM((1, wide), jnp.float32),
                pltpu.VMEM((1, wide), jnp.float32),
                pltpu.VMEM((1, wide), jnp.float32),
                pltpu.SemaphoreType.DMA((pieces,)),
            ],
        ),
        out_shape=jax.ShapeDtypeStruct(q_loc.shape, jnp.bfloat16),
        input_output_aliases=aliases,
        compiler_params=pltpu.CompilerParams(dimension_semantics=("arbitrary",), vmem_limit_bytes=48 * 1024 * 1024),
        cost_estimate=pl.CostEstimate(flops=pairs * q_heads * 4 * head_dim, bytes_accessed=heads * pieces * piece_len * head_dim * 4, transcendentals=pairs * q_heads),
    )(*operands)


def solution(mesh):
    size_cy = mesh.shape['cy']
    group = mesh.shape['cx'] * size_cy
    seq_spec = P(('dp', 'cx', 'cy'), None, None)
    doc_spec = P(('dp', 'cx', 'cy'))

    def per_device(q_loc, k_loc, v_loc, doc_loc):
        tok_dev, num_heads, head_dim = q_loc.shape
        kv_heads = k_loc.shape[1]
        piece_len = tok_dev // 2
        tiles = tok_dev // TILE
        rank = lax.axis_index('cx') * size_cy + lax.axis_index('cy')

        k_heads = k_loc.transpose(1, 0, 2)
        v_heads = v_loc.reshape(tok_dev // head_dim, head_dim, kv_heads, head_dim).transpose(2, 0, 3, 1).reshape(kv_heads, tok_dev, head_dim)
        gathered = []
        for head_lo in range(0, kv_heads, CHUNK):
            part = jnp.stack([k_heads[head_lo:head_lo + CHUNK], v_heads[head_lo:head_lo + CHUNK]])
            gathered.append(lax.all_gather(part, ('cx', 'cy')))

        below = jnp.sum(doc_loc[None, :] < jnp.arange(DOCS, dtype=jnp.int32)[:, None], axis=1, dtype=jnp.int32)
        below = lax.psum(below, ('cx', 'cy'))
        starts = jnp.zeros_like(doc_loc)
        for doc in range(DOCS):
            starts = jnp.where(doc_loc == doc, below[doc], starts)
        starts = starts.reshape(tiles, 1, TILE)
        tile_ids = jnp.arange(tiles, dtype=jnp.int32)
        half = tiles // 2
        tile_blk = jnp.where(tile_ids < half, rank * half + tile_ids, (2 * group - 1 - rank) * half + tile_ids - half).astype(jnp.int32)
        tab = jnp.stack([starts[:, 0, 0] // BLK, tile_blk, starts[:, 0, TILE - 1]])
        first_lo = starts[0, 0, 0] // piece_len
        second_lo = starts[half, 0, 0] // piece_len
        first_end = rank + 1
        rng = jnp.stack([jnp.stack([jnp.minimum(first_lo, second_lo), first_end]), jnp.stack([jnp.maximum(second_lo, first_end), 2 * group - rank])]).astype(jnp.int32)

        out = None
        for chunk, kv_all in enumerate(gathered):
            out = attend(tab, rng, kv_all, q_loc, starts, out, chunk)
        return out

    return jax.shard_map(per_device, mesh=mesh, in_specs=(seq_spec, seq_spec, seq_spec, doc_spec), out_specs=seq_spec, check_vma=False)
```

```python
import functools
import math

import jax
import jax.numpy as jnp
from jax import lax
from jax.experimental import pallas as pl
from jax.experimental.pallas import tpu as pltpu
from jax.sharding import PartitionSpec as P

DOCS = 6
TILE = 256
UNIT = 128
BLK_UNITS = 4
BLK = UNIT * BLK_UNITS
SUBLANES = 8
LANES = 128
CHUNK = 2
HEAD_DIM = 128
KV_HEADS = 8
SCALE_LOG2 = HEAD_DIM ** -0.5 * math.log2(math.e)
NEG_BIG = -1e30 * HEAD_DIM ** 0.5


def attend_kernel(tab_ref, rng_ref, kv_hbm, q_ref, q_next_ref, start_ref, *rest, heads, pieces, piece_len, q_per_kv):
    out_ref, kv_scr, q_scr, qt_scr, s_scr, p_scr, acc_scr, top_scr, max_scr, sum_scr, fac_scr, sems = rest[-12:]
    tile = pl.program_id(0)
    tiles_piece = piece_len // TILE
    q_heads = heads * q_per_kv
    halves = TILE // LANES

    def piece_copy(piece):
        upper = piece >= pieces // 2
        rank = jnp.where(upper, pieces - 1 - piece, piece)
        row = jnp.where(upper, piece_len, 0)
        return pltpu.make_async_copy(
            kv_hbm.at[rank, :, :, pl.ds(pl.multiple_of(row, piece_len), piece_len), :],
            kv_scr.at[:, :, pl.ds(pl.multiple_of(piece * piece_len + BLK, BLK), piece_len), :],
            sems.at[piece])

    def over_range(which, fn):
        def body(piece, _):
            fn(piece)
            return 0
        lax.fori_loop(rng_ref[which, 0], rng_ref[which, 1], body, 0)

    @pl.when(tile == 0)
    def _():
        over_range(0, lambda piece: piece_copy(piece).start())
        over_range(1, lambda piece: piece_copy(piece).start())
        kv_scr[:, :, :BLK, :] = jnp.zeros(kv_scr.shape[:2] + (BLK, HEAD_DIM), kv_scr.dtype)

    cur_slot = lax.rem(tile, 2)
    next_slot = 1 - cur_slot

    def turn_q(ref, slot):
        q_scr[...] = ref[...].astype(jnp.float32).reshape(TILE * q_heads, HEAD_DIM)
        for head in range(q_heads):
            q_head = q_scr[pl.ds(head, TILE, stride=q_heads), :].astype(jnp.bfloat16).T
            for half in range(halves):
                qt_scr[slot, head * halves + half] = q_head[:, half * LANES:(half + 1) * LANES]

    def span(tile_idx):
        tile_end = (tab_ref[1, tile_idx] + 1) * halves
        count = (tile_end - tab_ref[0, tile_idx] + BLK_UNITS - 1) // BLK_UNITS
        return tile_end - count * BLK_UNITS, tile_end, count

    tile_blk = tab_ref[1, tile]
    start_last = tab_ref[2, tile]
    unit_first, unit_end, blocks = span(tile)
    next_first, _, _ = span(jnp.minimum(tile + 1, pl.num_programs(0) - 1))

    def cols(head):
        return pl.ds(head * TILE, TILE)

    def rows(unit):
        return pl.ds(pl.multiple_of(unit * UNIT + BLK, UNIT), BLK)

    def part_max(scores):
        return jnp.max(scores.reshape(UNIT // SUBLANES, SUBLANES, TILE), axis=0)

    def score(k_blk, head, slot):
        q_head = jnp.concatenate([qt_scr[slot, head * halves + half] for half in range(halves)], axis=1)
        scores = jnp.dot(k_blk, q_head, preferred_element_type=jnp.float32)
        s_scr[:, cols(head)] = scores
        for sub in range(BLK_UNITS):
            top_scr[sub, :, cols(head)] = part_max(scores[sub * UNIT:(sub + 1) * UNIT])

    def load_v(kv_head, unit):
        v_blk = kv_scr[1, kv_head, rows(unit), :]
        return jnp.concatenate([v_blk[i * HEAD_DIM:(i + 1) * HEAD_DIM] for i in range(BLK // HEAD_DIM)], axis=1)

    def product(v_blk, head):
        p_head = jnp.concatenate([p_scr[head * halves + half] for half in range(halves)], axis=1)
        acc_scr[:, cols(head)] = acc_scr[:, cols(head)] * fac_scr[:, cols(head)] + jnp.dot(v_blk, p_head, preferred_element_type=jnp.float32)

    def soften(head):
        max_old = max_scr[:, cols(head)]
        top = jnp.max(jnp.max(top_scr[:, :, cols(head)], axis=0), axis=0, keepdims=True)
        max_new = jnp.maximum(max_old, top)
        fac = jnp.exp2((max_old - max_new) * SCALE_LOG2)
        max_scr[:, cols(head)] = max_new
        fac_scr[:, cols(head)] = fac
        weights = jnp.exp2((s_scr[:, cols(head)] - max_new) * SCALE_LOG2)
        sum_scr[:, cols(head)] = sum_scr[:, cols(head)] * fac + jnp.sum(weights.reshape(BLK // SUBLANES, SUBLANES, TILE), axis=0)
        for half in range(halves):
            p_scr[head * halves + half] = weights[:, half * LANES:(half + 1) * LANES].astype(jnp.bfloat16)

    @pl.when(tile == 0)
    def _():
        p_scr[...] = jnp.zeros_like(p_scr)
        turn_q(q_ref, 0)
        over_range(0, lambda piece: piece_copy(piece).wait())
        for kv_head in range(heads):
            k_first = kv_scr[0, kv_head, rows(unit_first), :]
            for col in range(q_per_kv):
                score(k_first, kv_head * q_per_kv + col, 0)

    @pl.when(tile == tiles_piece - 1)
    def _():
        over_range(1, lambda piece: piece_copy(piece).wait())

    turn_q(q_next_ref, next_slot)
    acc_scr[...] = jnp.zeros_like(acc_scr)
    fac_scr[...] = jnp.zeros_like(fac_scr)
    sum_scr[...] = jnp.zeros_like(sum_scr)
    max_scr[...] = jnp.full_like(max_scr, NEG_BIG)

    def step(idx, _):
        unit = unit_first + idx * BLK_UNITS

        @pl.when((idx == blocks - 1) | (unit * UNIT < start_last))
        def _():
            def mask_unit(sub, _):
                cur = unit + sub

                @pl.when((cur >= unit_end - halves) | (cur * UNIT < start_last))
                def _():
                    k_pos = cur * UNIT + lax.broadcasted_iota(jnp.int32, (UNIT, TILE), 0)
                    q_pos = tile_blk * TILE + lax.broadcasted_iota(jnp.int32, (UNIT, TILE), 1)
                    allowed = (k_pos <= q_pos) & (k_pos >= start_ref[0])
                    sub_rows = pl.ds(pl.multiple_of(sub * UNIT, UNIT), UNIT)
                    for head in range(q_heads):
                        scores = jnp.where(allowed, s_scr[sub_rows, cols(head)], NEG_BIG)
                        s_scr[sub_rows, cols(head)] = scores
                        top_scr[sub, :, cols(head)] = part_max(scores)
                return 0
            lax.fori_loop(0, BLK_UNITS, mask_unit, 0)

        last = idx == blocks - 1
        unit_next = jnp.where(last, next_first, unit + BLK_UNITS)
        q_slot = jnp.where(last, next_slot, cur_slot)
        for kv_head in range(heads):
            v_prev = load_v(kv_head, jnp.where(idx == 0, -BLK_UNITS, unit - BLK_UNITS))
            k_next = kv_scr[0, kv_head, rows(unit_next), :]
            for col in range(q_per_kv):
                head = kv_head * q_per_kv + col
                product(v_prev, head)
                soften(head)
                score(k_next, head, q_slot)
        return 0

    lax.fori_loop(0, blocks, step, 0)
    for kv_head in range(heads):
        v_last = load_v(kv_head, unit_end - BLK_UNITS)
        for col in range(q_per_kv):
            head = kv_head * q_per_kv + col
            product(v_last, head)
            normed = acc_scr[:, cols(head)] * (1.0 / jnp.sum(sum_scr[:, cols(head)], axis=0, keepdims=True))
            q_scr[pl.ds(head, TILE, stride=q_heads), :] = normed.astype(jnp.bfloat16).T.astype(jnp.float32)
    out_ref[...] = q_scr[...].reshape(TILE, q_heads, HEAD_DIM).astype(jnp.bfloat16)


def attend(tab, rng, kv_all, q_loc, starts, prev, chunk):
    ranks, _, heads, tok_dev, head_dim = kv_all.shape
    num_heads = q_loc.shape[1]
    pieces = 2 * ranks
    piece_len = tok_dev // 2
    tiles = tok_dev // TILE
    q_per_kv = num_heads // KV_HEADS
    q_heads = heads * q_per_kv
    wide = q_heads * TILE
    body = functools.partial(attend_kernel, heads=heads, pieces=pieces, piece_len=piece_len, q_per_kv=q_per_kv)
    pairs = ranks * tok_dev * tok_dev // 4
    operands = [tab, rng, kv_all, q_loc, q_loc, starts]
    in_specs = [
        pl.BlockSpec(memory_space=pl.ANY),
        pl.BlockSpec((TILE, q_heads, head_dim), lambda t, *_: (0, chunk, 0)),
        pl.BlockSpec((TILE, q_heads, head_dim), lambda t, *_: (jnp.minimum(t + 1, tiles - 1), chunk, 0)),
        pl.BlockSpec((1, 1, TILE), lambda t, *_: (t, 0, 0)),
    ]
    aliases = {}
    if prev is not None:
        operands.append(prev)
        in_specs.append(pl.BlockSpec(memory_space=pl.ANY))
        aliases = {6: 0}
    return pl.pallas_call(
        body,
        grid_spec=pltpu.PrefetchScalarGridSpec(
            num_scalar_prefetch=2,
            grid=(tiles,),
            in_specs=in_specs,
            out_specs=pl.BlockSpec((TILE, q_heads, head_dim), lambda t, *_: (t, chunk, 0)),
            scratch_shapes=[
                pltpu.VMEM((2, heads, pieces * piece_len + BLK, head_dim), jnp.bfloat16),
                pltpu.VMEM((TILE * q_heads, head_dim), jnp.float32),
                pltpu.VMEM((2, wide // LANES, head_dim, LANES), jnp.bfloat16),
                pltpu.VMEM((BLK, wide), jnp.float32),
                pltpu.VMEM((wide // LANES, BLK, LANES), jnp.bfloat16),
                pltpu.VMEM((head_dim, wide), jnp.float32),
                pltpu.VMEM((BLK_UNITS, SUBLANES, wide), jnp.float32),
                pltpu.VMEM((1, wide), jnp.float32),
                pltpu.VMEM((SUBLANES, wide), jnp.float32),
                pltpu.VMEM((1, wide), jnp.float32),
                pltpu.SemaphoreType.DMA((pieces,)),
            ],
        ),
        out_shape=jax.ShapeDtypeStruct(q_loc.shape, jnp.bfloat16),
        input_output_aliases=aliases,
        compiler_params=pltpu.CompilerParams(dimension_semantics=("arbitrary",), vmem_limit_bytes=48 * 1024 * 1024),
        cost_estimate=pl.CostEstimate(flops=pairs * q_heads * 4 * head_dim, bytes_accessed=heads * pieces * piece_len * head_dim * 4, transcendentals=pairs * q_heads),
    )(*operands)


def solution(mesh):
    size_cy = mesh.shape['cy']
    group = mesh.shape['cx'] * size_cy
    seq_spec = P(('dp', 'cx', 'cy'), None, None)
    doc_spec = P(('dp', 'cx', 'cy'))

    def per_device(q_loc, k_loc, v_loc, doc_loc):
        tok_dev, num_heads, head_dim = q_loc.shape
        kv_heads = k_loc.shape[1]
        piece_len = tok_dev // 2
        tiles = tok_dev // TILE
        rank = lax.axis_index('cx') * size_cy + lax.axis_index('cy')

        k_heads = k_loc.transpose(1, 0, 2)
        v_heads = v_loc.reshape(tok_dev // head_dim, head_dim, kv_heads, head_dim).transpose(2, 0, 3, 1).reshape(kv_heads, tok_dev, head_dim)
        gathered = []
        for head_lo in range(0, kv_heads, CHUNK):
            part = jnp.stack([k_heads[head_lo:head_lo + CHUNK], v_heads[head_lo:head_lo + CHUNK]])
            gathered.append(lax.all_gather(part, ('cx', 'cy')))

        below = jnp.sum(doc_loc[None, :] < jnp.arange(DOCS, dtype=jnp.int32)[:, None], axis=1, dtype=jnp.int32)
        below = lax.psum(below, ('cx', 'cy'))
        starts = jnp.zeros_like(doc_loc)
        for doc in range(DOCS):
            starts = jnp.where(doc_loc == doc, below[doc], starts)
        starts = starts.reshape(tiles, 1, TILE)
        tile_ids = jnp.arange(tiles, dtype=jnp.int32)
        half = tiles // 2
        tile_blk = jnp.where(tile_ids < half, rank * half + tile_ids, (2 * group - 1 - rank) * half + tile_ids - half).astype(jnp.int32)
        tab = jnp.stack([starts[:, 0, 0] // UNIT, tile_blk, starts[:, 0, TILE - 1]])
        first_lo = jnp.maximum(starts[0, 0, 0] - (BLK - UNIT), 0) // piece_len
        second_lo = jnp.maximum(starts[half, 0, 0] - (BLK - UNIT), 0) // piece_len
        first_end = rank + 1
        rng = jnp.stack([jnp.stack([jnp.minimum(first_lo, second_lo), first_end]), jnp.stack([jnp.maximum(second_lo, first_end), 2 * group - rank])]).astype(jnp.int32)

        out = None
        for chunk, kv_all in enumerate(gathered):
            out = attend(tab, rng, kv_all, q_loc, starts, out, chunk)
        return out

    return jax.shard_map(per_device, mesh=mesh, in_specs=(seq_spec, seq_spec, seq_spec, doc_spec), out_specs=seq_spec, check_vma=False)
```

```python
import functools
import math

import jax
import jax.numpy as jnp
from jax import lax
from jax.experimental import pallas as pl
from jax.experimental.pallas import tpu as pltpu
from jax.sharding import PartitionSpec as P

DOCS = 6
TILE = 256
UNIT = 128
BLK_UNITS = 4
BLK = UNIT * BLK_UNITS
SUBLANES = 8
LANES = 128
CHUNKS = ((0, 2), (2, 2), (4, 2), (6, 2))
HEAD_BLOCK = 8
HEAD_DIM = 128
KV_HEADS = 8
SCALE_LOG2 = HEAD_DIM ** -0.5 * math.log2(math.e)
NEG_BIG = -1e30 * HEAD_DIM ** 0.5


def attend_kernel(tab_ref, rng_ref, kv_hbm, q_ref, q_next_ref, start_ref, *rest, heads, pieces, piece_len, q_per_kv, head_lo, merge):
    prev_ref = rest[0]
    out_ref, kv_scr, q_scr, qt_scr, s_scr, p_scr, acc_scr, top_scr, max_scr, sum_scr, fac_scr, sems = rest[-12:]
    tile = pl.program_id(0)
    tiles_piece = piece_len // TILE
    q_heads = heads * q_per_kv
    halves = TILE // LANES

    def piece_copy(piece):
        upper = piece >= pieces // 2
        rank = jnp.where(upper, pieces - 1 - piece, piece)
        row = jnp.where(upper, piece_len, 0)
        return pltpu.make_async_copy(
            kv_hbm.at[rank, :, :, pl.ds(pl.multiple_of(row, piece_len), piece_len), :],
            kv_scr.at[:, :, pl.ds(pl.multiple_of(piece * piece_len + BLK, BLK), piece_len), :],
            sems.at[piece])

    def over_range(which, fn):
        def body(piece, _):
            fn(piece)
            return 0
        lax.fori_loop(rng_ref[which, 0], rng_ref[which, 1], body, 0)

    @pl.when(tile == 0)
    def _():
        over_range(0, lambda piece: piece_copy(piece).start())
        kv_scr[:, :, :BLK, :] = jnp.zeros(kv_scr.shape[:2] + (BLK, HEAD_DIM), kv_scr.dtype)

    cur_slot = lax.rem(tile, 2)
    next_slot = 1 - cur_slot

    def turn_q(ref, slot):
        q_scr[...] = ref[...].astype(jnp.float32).reshape(TILE * HEAD_BLOCK, HEAD_DIM)
        for head in range(q_heads):
            q_head = q_scr[pl.ds(head_lo + head, TILE, stride=HEAD_BLOCK), :].astype(jnp.bfloat16).T
            for half in range(halves):
                qt_scr[slot, head * halves + half] = q_head[:, half * LANES:(half + 1) * LANES]

    def span(tile_idx):
        tile_end = (tab_ref[1, tile_idx] + 1) * halves
        count = (tile_end - tab_ref[0, tile_idx] + BLK_UNITS - 1) // BLK_UNITS
        return tile_end - count * BLK_UNITS, tile_end, count

    tile_blk = tab_ref[1, tile]
    start_last = tab_ref[2, tile]
    unit_first, unit_end, blocks = span(tile)
    next_first, _, _ = span(jnp.minimum(tile + 1, pl.num_programs(0) - 1))

    def cols(head):
        return pl.ds(head * TILE, TILE)

    def rows(unit):
        return pl.ds(pl.multiple_of(unit * UNIT + BLK, UNIT), BLK)

    def part_max(scores):
        return jnp.max(scores.reshape(UNIT // SUBLANES, SUBLANES, TILE), axis=0)

    def score(k_blk, head, slot):
        q_head = jnp.concatenate([qt_scr[slot, head * halves + half] for half in range(halves)], axis=1)
        scores = jnp.dot(k_blk, q_head, preferred_element_type=jnp.float32)
        s_scr[:, cols(head)] = scores
        for sub in range(BLK_UNITS):
            top_scr[sub, :, cols(head)] = part_max(scores[sub * UNIT:(sub + 1) * UNIT])

    def load_v(kv_head, unit):
        v_blk = kv_scr[1, kv_head, rows(unit), :]
        return jnp.concatenate([v_blk[i * HEAD_DIM:(i + 1) * HEAD_DIM] for i in range(BLK // HEAD_DIM)], axis=1)

    def product(v_blk, head):
        p_head = jnp.concatenate([p_scr[head * halves + half] for half in range(halves)], axis=1)
        acc_scr[:, cols(head)] = acc_scr[:, cols(head)] * fac_scr[:, cols(head)] + jnp.dot(v_blk, p_head, preferred_element_type=jnp.float32)

    def soften(head):
        max_old = max_scr[:, cols(head)]
        top = jnp.max(jnp.max(top_scr[:, :, cols(head)], axis=0), axis=0, keepdims=True)
        max_new = jnp.maximum(max_old, top)
        fac = jnp.exp2((max_old - max_new) * SCALE_LOG2)
        max_scr[:, cols(head)] = max_new
        fac_scr[:, cols(head)] = fac
        weights = jnp.exp2((s_scr[:, cols(head)] - max_new) * SCALE_LOG2)
        sum_scr[:, cols(head)] = sum_scr[:, cols(head)] * fac + jnp.sum(weights.reshape(BLK // SUBLANES, SUBLANES, TILE), axis=0)
        for half in range(halves):
            p_scr[head * halves + half] = weights[:, half * LANES:(half + 1) * LANES].astype(jnp.bfloat16)

    @pl.when(tile == 0)
    def _():
        p_scr[...] = jnp.zeros_like(p_scr)
        turn_q(q_ref, 0)
        over_range(0, lambda piece: piece_copy(piece).wait())
        over_range(1, lambda piece: piece_copy(piece).start())
        for kv_head in range(heads):
            k_first = kv_scr[0, kv_head, rows(unit_first), :]
            for col in range(q_per_kv):
                score(k_first, kv_head * q_per_kv + col, 0)

    @pl.when(tile == tiles_piece - 1)
    def _():
        over_range(1, lambda piece: piece_copy(piece).wait())

    turn_q(q_next_ref, next_slot)
    acc_scr[...] = jnp.zeros_like(acc_scr)
    fac_scr[...] = jnp.zeros_like(fac_scr)
    sum_scr[...] = jnp.zeros_like(sum_scr)
    max_scr[...] = jnp.full_like(max_scr, NEG_BIG)

    def step(idx, _):
        unit = unit_first + idx * BLK_UNITS

        @pl.when((idx == blocks - 1) | (unit * UNIT < start_last))
        def _():
            def mask_unit(sub, _):
                cur = unit + sub

                @pl.when((cur >= unit_end - halves) | (cur * UNIT < start_last))
                def _():
                    k_pos = cur * UNIT + lax.broadcasted_iota(jnp.int32, (UNIT, TILE), 0)
                    q_pos = tile_blk * TILE + lax.broadcasted_iota(jnp.int32, (UNIT, TILE), 1)
                    allowed = (k_pos <= q_pos) & (k_pos >= start_ref[0])
                    sub_rows = pl.ds(pl.multiple_of(sub * UNIT, UNIT), UNIT)
                    for head in range(q_heads):
                        scores = jnp.where(allowed, s_scr[sub_rows, cols(head)], NEG_BIG)
                        s_scr[sub_rows, cols(head)] = scores
                        top_scr[sub, :, cols(head)] = part_max(scores)
                return 0
            lax.fori_loop(0, BLK_UNITS, mask_unit, 0)

        last = idx == blocks - 1
        unit_next = jnp.where(last, next_first, unit + BLK_UNITS)
        q_slot = jnp.where(last, next_slot, cur_slot)
        for kv_head in range(heads):
            v_prev = load_v(kv_head, jnp.where(idx == 0, -BLK_UNITS, unit - BLK_UNITS))
            k_next = kv_scr[0, kv_head, rows(unit_next), :]
            for col in range(q_per_kv):
                head = kv_head * q_per_kv + col
                product(v_prev, head)
                soften(head)
                score(k_next, head, q_slot)
        return 0

    lax.fori_loop(0, blocks, step, 0)
    if merge:
        q_scr[...] = prev_ref[...].astype(jnp.float32).reshape(TILE * HEAD_BLOCK, HEAD_DIM)
    for kv_head in range(heads):
        v_last = load_v(kv_head, unit_end - BLK_UNITS)
        for col in range(q_per_kv):
            head = kv_head * q_per_kv + col
            product(v_last, head)
            normed = acc_scr[:, cols(head)] * (1.0 / jnp.sum(sum_scr[:, cols(head)], axis=0, keepdims=True))
            q_scr[pl.ds(head_lo + head, TILE, stride=HEAD_BLOCK), :] = normed.astype(jnp.bfloat16).T.astype(jnp.float32)
    out_ref[...] = q_scr[...].reshape(TILE, HEAD_BLOCK, HEAD_DIM).astype(jnp.bfloat16)


def attend(tab, rng, kv_all, q_loc, starts, prev, first_head):
    ranks, _, heads, tok_dev, head_dim = kv_all.shape
    num_heads = q_loc.shape[1]
    pieces = 2 * ranks
    piece_len = tok_dev // 2
    tiles = tok_dev // TILE
    q_per_kv = num_heads // KV_HEADS
    q_heads = heads * q_per_kv
    wide = q_heads * TILE
    head_blk, head_lo = divmod(first_head * q_per_kv, HEAD_BLOCK)
    merge = head_lo > 0
    block = (TILE, HEAD_BLOCK, head_dim)
    body = functools.partial(attend_kernel, heads=heads, pieces=pieces, piece_len=piece_len, q_per_kv=q_per_kv, head_lo=head_lo, merge=merge)
    pairs = ranks * tok_dev * tok_dev // 4
    operands = [tab, rng, kv_all, q_loc, q_loc, starts]
    in_specs = [
        pl.BlockSpec(memory_space=pl.ANY),
        pl.BlockSpec(block, lambda t, *_: (0, head_blk, 0)),
        pl.BlockSpec(block, lambda t, *_: (jnp.minimum(t + 1, tiles - 1), head_blk, 0)),
        pl.BlockSpec((1, 1, TILE), lambda t, *_: (t, 0, 0)),
    ]
    aliases = {}
    if prev is not None:
        operands.append(prev)
        in_specs.append(pl.BlockSpec(block, lambda t, *_: (t, head_blk, 0)) if merge else pl.BlockSpec(memory_space=pl.ANY))
        aliases = {6: 0}
    return pl.pallas_call(
        body,
        grid_spec=pltpu.PrefetchScalarGridSpec(
            num_scalar_prefetch=2,
            grid=(tiles,),
            in_specs=in_specs,
            out_specs=pl.BlockSpec(block, lambda t, *_: (t, head_blk, 0)),
            scratch_shapes=[
                pltpu.VMEM((2, heads, pieces * piece_len + BLK, head_dim), jnp.bfloat16),
                pltpu.VMEM((TILE * HEAD_BLOCK, head_dim), jnp.float32),
                pltpu.VMEM((2, wide // LANES, head_dim, LANES), jnp.bfloat16),
                pltpu.VMEM((BLK, wide), jnp.float32),
                pltpu.VMEM((wide // LANES, BLK, LANES), jnp.bfloat16),
                pltpu.VMEM((head_dim, wide), jnp.float32),
                pltpu.VMEM((BLK_UNITS, SUBLANES, wide), jnp.float32),
                pltpu.VMEM((1, wide), jnp.float32),
                pltpu.VMEM((SUBLANES, wide), jnp.float32),
                pltpu.VMEM((1, wide), jnp.float32),
                pltpu.SemaphoreType.DMA((pieces,)),
            ],
        ),
        out_shape=jax.ShapeDtypeStruct(q_loc.shape, jnp.bfloat16),
        input_output_aliases=aliases,
        compiler_params=pltpu.CompilerParams(dimension_semantics=("arbitrary",), vmem_limit_bytes=48 * 1024 * 1024),
        cost_estimate=pl.CostEstimate(flops=pairs * q_heads * 4 * head_dim, bytes_accessed=heads * pieces * piece_len * head_dim * 4, transcendentals=pairs * q_heads),
    )(*operands)


def solution(mesh):
    size_cy = mesh.shape['cy']
    group = mesh.shape['cx'] * size_cy
    seq_spec = P(('dp', 'cx', 'cy'), None, None)
    doc_spec = P(('dp', 'cx', 'cy'))

    def per_device(q_loc, k_loc, v_loc, doc_loc):
        tok_dev, num_heads, head_dim = q_loc.shape
        kv_heads = k_loc.shape[1]
        piece_len = tok_dev // 2
        tiles = tok_dev // TILE
        rank = lax.axis_index('cx') * size_cy + lax.axis_index('cy')

        def gather(k_src, v_src, first_head, heads):
            k_part = k_src[:, first_head:first_head + heads].transpose(1, 0, 2)
            v_part = v_src[:, first_head:first_head + heads].reshape(tok_dev // head_dim, head_dim, heads, head_dim).transpose(2, 0, 3, 1)
            part = jnp.stack([k_part, v_part.reshape(heads, tok_dev, head_dim)])
            return lax.all_gather(part, ('cx', 'cy'))

        gathered = [gather(k_loc, v_loc, *CHUNKS[0])]
        below = jnp.sum(doc_loc[None, :] < jnp.arange(DOCS, dtype=jnp.int32)[:, None], axis=1, dtype=jnp.int32)
        below = lax.psum(below, ('cx', 'cy'))
        below, k_rest, v_rest = lax.optimization_barrier((below, k_loc, v_loc))
        gathered += [gather(k_rest, v_rest, *chunk) for chunk in CHUNKS[1:]]
        starts = jnp.zeros_like(doc_loc)
        for doc in range(DOCS):
            starts = jnp.where(doc_loc == doc, below[doc], starts)
        starts = starts.reshape(tiles, 1, TILE)
        tile_ids = jnp.arange(tiles, dtype=jnp.int32)
        half = tiles // 2
        tile_blk = jnp.where(tile_ids < half, rank * half + tile_ids, (2 * group - 1 - rank) * half + tile_ids - half).astype(jnp.int32)
        tab = jnp.stack([starts[:, 0, 0] // UNIT, tile_blk, starts[:, 0, TILE - 1]])
        first_lo = jnp.maximum(starts[0, 0, 0] - (BLK - UNIT), 0) // piece_len
        second_lo = jnp.maximum(starts[half, 0, 0] - (BLK - UNIT), 0) // piece_len
        first_end = rank + 1
        rng = jnp.stack([jnp.stack([jnp.minimum(first_lo, second_lo), first_end]), jnp.stack([jnp.maximum(second_lo, first_end), 2 * group - rank])]).astype(jnp.int32)

        out = None
        for (first_head, _), kv_all in zip(CHUNKS, gathered):
            out = attend(tab, rng, kv_all, q_loc, starts, out, first_head)
        return out

    return jax.shard_map(per_device, mesh=mesh, in_specs=(seq_spec, seq_spec, seq_spec, doc_spec), out_specs=seq_spec, check_vma=False)
```

```python
import functools
import math

import jax
import jax.numpy as jnp
from jax import lax
from jax.experimental import pallas as pl
from jax.experimental.pallas import tpu as pltpu
from jax.sharding import PartitionSpec as P

DOCS = 6
TILE = 256
UNIT = 128
BLK_UNITS = 4
BLK = UNIT * BLK_UNITS
SUBLANES = 8
LANES = 128
CHUNKS = ((0, 2), (2, 2), (4, 2), (6, 2))
HEAD_BLOCK = 8
HEAD_DIM = 128
KV_HEADS = 8
SCALE_LOG2 = HEAD_DIM ** -0.5 * math.log2(math.e)
NEG_BIG = -1e30 * HEAD_DIM ** 0.5


def attend_kernel(tab_ref, rng_ref, kv_hbm, q_ref, q_second_ref, q_next_ref, start_ref, *rest, heads, pieces, piece_len, q_per_kv, head_lo, merge):
    prev_ref = rest[0]
    out_ref, kv_scr, q_scr, turn_scr, qt_scr, s_scr, p_scr, acc_scr, top_scr, max_scr, sum_scr, fac_scr, sems = rest[-13:]
    tile = pl.program_id(0)
    tiles_piece = piece_len // TILE
    q_heads = heads * q_per_kv
    halves = TILE // LANES

    def piece_copy(piece):
        upper = piece >= pieces // 2
        rank = jnp.where(upper, pieces - 1 - piece, piece)
        row = jnp.where(upper, piece_len, 0)
        return pltpu.make_async_copy(
            kv_hbm.at[rank, :, :, pl.ds(pl.multiple_of(row, piece_len), piece_len), :],
            kv_scr.at[:, :, pl.ds(pl.multiple_of(piece * piece_len + BLK, BLK), piece_len), :],
            sems.at[piece])

    def over_range(which, fn):
        def body(piece, _):
            fn(piece)
            return 0
        lax.fori_loop(rng_ref[which, 0], rng_ref[which, 1], body, 0)

    @pl.when(tile == 0)
    def _():
        over_range(0, lambda piece: piece_copy(piece).start())
        kv_scr[:, :, :BLK, :] = jnp.zeros(kv_scr.shape[:2] + (BLK, HEAD_DIM), kv_scr.dtype)

    cur_slot = lax.rem(tile, 2)
    next_slot = 1 - cur_slot

    def turn_q(ref, slot):
        turn_scr[...] = ref[...].astype(jnp.float32).reshape(TILE * HEAD_BLOCK, HEAD_DIM)
        for head in range(q_heads):
            q_head = turn_scr[pl.ds(head_lo + head, TILE, stride=HEAD_BLOCK), :].astype(jnp.bfloat16).T
            for half in range(halves):
                qt_scr[slot, head * halves + half] = q_head[:, half * LANES:(half + 1) * LANES]

    def span(tile_idx):
        tile_end = (tab_ref[1, tile_idx] + 1) * halves
        count = (tile_end - tab_ref[0, tile_idx] + BLK_UNITS - 1) // BLK_UNITS
        return tile_end - count * BLK_UNITS, tile_end, count

    tile_blk = tab_ref[1, tile]
    start_last = tab_ref[2, tile]
    unit_first, unit_end, blocks = span(tile)
    next_first, _, _ = span(jnp.minimum(tile + 1, pl.num_programs(0) - 1))

    def cols(head):
        return pl.ds(head * TILE, TILE)

    def rows(unit):
        return pl.ds(pl.multiple_of(unit * UNIT + BLK, UNIT), BLK)

    def part_max(scores):
        return jnp.max(scores.reshape(UNIT // SUBLANES, SUBLANES, TILE), axis=0)

    def score(k_blk, head, slot):
        q_head = jnp.concatenate([qt_scr[slot, head * halves + half] for half in range(halves)], axis=1)
        scores = jnp.dot(k_blk, q_head, preferred_element_type=jnp.float32)
        s_scr[:, cols(head)] = scores
        for sub in range(BLK_UNITS):
            top_scr[sub, :, cols(head)] = part_max(scores[sub * UNIT:(sub + 1) * UNIT])

    def load_v(kv_head, unit):
        v_blk = kv_scr[1, kv_head, rows(unit), :]
        return jnp.concatenate([v_blk[i * HEAD_DIM:(i + 1) * HEAD_DIM] for i in range(BLK // HEAD_DIM)], axis=1)

    def weigh(v_blk, head):
        p_head = jnp.concatenate([p_scr[head * halves + half] for half in range(halves)], axis=1)
        return jnp.dot(v_blk, p_head, preferred_element_type=jnp.float32)

    def product(v_blk, head):
        acc_scr[:, cols(head)] = acc_scr[:, cols(head)] * fac_scr[:, cols(head)] + weigh(v_blk, head)

    def soften(head):
        max_old = max_scr[:, cols(head)]
        top = jnp.max(jnp.max(top_scr[:, :, cols(head)], axis=0), axis=0, keepdims=True)
        max_new = jnp.maximum(max_old, top)
        fac = jnp.exp2((max_old - max_new) * SCALE_LOG2)
        max_scr[:, cols(head)] = max_new
        fac_scr[:, cols(head)] = fac
        weights = jnp.exp2((s_scr[:, cols(head)] - max_new) * SCALE_LOG2)
        sum_scr[:, cols(head)] = sum_scr[:, cols(head)] * fac + jnp.sum(weights.reshape(BLK // SUBLANES, SUBLANES, TILE), axis=0)
        for half in range(halves):
            p_scr[head * halves + half] = weights[:, half * LANES:(half + 1) * LANES].astype(jnp.bfloat16)

    @pl.when(tile == 0)
    def _():
        p_scr[...] = jnp.zeros_like(p_scr)
        turn_q(q_ref, 0)
        turn_q(q_second_ref, 1)
        over_range(0, lambda piece: piece_copy(piece).wait())
        over_range(1, lambda piece: piece_copy(piece).start())
        for kv_head in range(heads):
            k_first = kv_scr[0, kv_head, rows(unit_first), :]
            for col in range(q_per_kv):
                score(k_first, kv_head * q_per_kv + col, 0)

    @pl.when(tile == tiles_piece - 1)
    def _():
        over_range(1, lambda piece: piece_copy(piece).wait())

    acc_scr[...] = jnp.zeros_like(acc_scr)
    fac_scr[...] = jnp.zeros_like(fac_scr)
    sum_scr[...] = jnp.zeros_like(sum_scr)
    max_scr[...] = jnp.full_like(max_scr, NEG_BIG)

    def step(idx, _):
        unit = unit_first + idx * BLK_UNITS

        @pl.when((idx == blocks - 1) | (unit * UNIT < start_last))
        def _():
            def mask_unit(sub, _):
                cur = unit + sub

                @pl.when((cur >= unit_end - halves) | (cur * UNIT < start_last))
                def _():
                    k_pos = cur * UNIT + lax.broadcasted_iota(jnp.int32, (UNIT, TILE), 0)
                    q_pos = tile_blk * TILE + lax.broadcasted_iota(jnp.int32, (UNIT, TILE), 1)
                    allowed = (k_pos <= q_pos) & (k_pos >= start_ref[0])
                    sub_rows = pl.ds(pl.multiple_of(sub * UNIT, UNIT), UNIT)
                    for head in range(q_heads):
                        scores = jnp.where(allowed, s_scr[sub_rows, cols(head)], NEG_BIG)
                        s_scr[sub_rows, cols(head)] = scores
                        top_scr[sub, :, cols(head)] = part_max(scores)
                return 0
            lax.fori_loop(0, BLK_UNITS, mask_unit, 0)

        last = idx == blocks - 1
        unit_next = jnp.where(last, next_first, unit + BLK_UNITS)
        q_slot = jnp.where(last, next_slot, cur_slot)
        for kv_head in range(heads):
            v_prev = load_v(kv_head, jnp.where(idx == 0, -BLK_UNITS, unit - BLK_UNITS))
            k_next = kv_scr[0, kv_head, rows(unit_next), :]
            for col in range(q_per_kv):
                head = kv_head * q_per_kv + col
                product(v_prev, head)
                soften(head)
                score(k_next, head, q_slot)
        return 0

    lax.fori_loop(0, blocks, step, 0)
    turn_q(q_next_ref, cur_slot)
    if merge:
        q_scr[...] = prev_ref[...].astype(jnp.float32).reshape(TILE * HEAD_BLOCK, HEAD_DIM)
    for kv_head in range(heads):
        v_last = load_v(kv_head, unit_end - BLK_UNITS)
        for col in range(q_per_kv):
            head = kv_head * q_per_kv + col
            total = acc_scr[:, cols(head)] * fac_scr[:, cols(head)] + weigh(v_last, head)
            normed = total * (1.0 / jnp.sum(sum_scr[:, cols(head)], axis=0, keepdims=True))
            q_scr[pl.ds(head_lo + head, TILE, stride=HEAD_BLOCK), :] = normed.astype(jnp.bfloat16).T.astype(jnp.float32)
    out_ref[...] = q_scr[...].reshape(TILE, HEAD_BLOCK, HEAD_DIM).astype(jnp.bfloat16)


def attend(tab, rng, kv_all, q_loc, starts, prev, first_head):
    ranks, _, heads, tok_dev, head_dim = kv_all.shape
    num_heads = q_loc.shape[1]
    pieces = 2 * ranks
    piece_len = tok_dev // 2
    tiles = tok_dev // TILE
    q_per_kv = num_heads // KV_HEADS
    q_heads = heads * q_per_kv
    wide = q_heads * TILE
    head_blk, head_lo = divmod(first_head * q_per_kv, HEAD_BLOCK)
    merge = head_lo > 0
    block = (TILE, HEAD_BLOCK, head_dim)
    body = functools.partial(attend_kernel, heads=heads, pieces=pieces, piece_len=piece_len, q_per_kv=q_per_kv, head_lo=head_lo, merge=merge)
    pairs = ranks * tok_dev * tok_dev // 4
    operands = [tab, rng, kv_all, q_loc, q_loc, q_loc, starts]
    in_specs = [
        pl.BlockSpec(memory_space=pl.ANY),
        pl.BlockSpec(block, lambda t, *_: (0, head_blk, 0)),
        pl.BlockSpec(block, lambda t, *_: (1, head_blk, 0)),
        pl.BlockSpec(block, lambda t, *_: (jnp.minimum(t + 2, tiles - 1), head_blk, 0)),
        pl.BlockSpec((1, 1, TILE), lambda t, *_: (t, 0, 0)),
    ]
    aliases = {}
    if prev is not None:
        operands.append(prev)
        in_specs.append(pl.BlockSpec(block, lambda t, *_: (t, head_blk, 0)) if merge else pl.BlockSpec(memory_space=pl.ANY))
        aliases = {7: 0}
    return pl.pallas_call(
        body,
        grid_spec=pltpu.PrefetchScalarGridSpec(
            num_scalar_prefetch=2,
            grid=(tiles,),
            in_specs=in_specs,
            out_specs=pl.BlockSpec(block, lambda t, *_: (t, head_blk, 0)),
            scratch_shapes=[
                pltpu.VMEM((2, heads, pieces * piece_len + BLK, head_dim), jnp.bfloat16),
                pltpu.VMEM((TILE * HEAD_BLOCK, head_dim), jnp.float32),
                pltpu.VMEM((TILE * HEAD_BLOCK, head_dim), jnp.float32),
                pltpu.VMEM((2, wide // LANES, head_dim, LANES), jnp.bfloat16),
                pltpu.VMEM((BLK, wide), jnp.float32),
                pltpu.VMEM((wide // LANES, BLK, LANES), jnp.bfloat16),
                pltpu.VMEM((head_dim, wide), jnp.float32),
                pltpu.VMEM((BLK_UNITS, SUBLANES, wide), jnp.float32),
                pltpu.VMEM((1, wide), jnp.float32),
                pltpu.VMEM((SUBLANES, wide), jnp.float32),
                pltpu.VMEM((1, wide), jnp.float32),
                pltpu.SemaphoreType.DMA((pieces,)),
            ],
        ),
        out_shape=jax.ShapeDtypeStruct(q_loc.shape, jnp.bfloat16),
        input_output_aliases=aliases,
        compiler_params=pltpu.CompilerParams(dimension_semantics=("arbitrary",), vmem_limit_bytes=48 * 1024 * 1024),
        cost_estimate=pl.CostEstimate(flops=pairs * q_heads * 4 * head_dim, bytes_accessed=heads * pieces * piece_len * head_dim * 4, transcendentals=pairs * q_heads),
    )(*operands)


def solution(mesh):
    size_cy = mesh.shape['cy']
    group = mesh.shape['cx'] * size_cy
    seq_spec = P(('dp', 'cx', 'cy'), None, None)
    doc_spec = P(('dp', 'cx', 'cy'))

    def per_device(q_loc, k_loc, v_loc, doc_loc):
        tok_dev, num_heads, head_dim = q_loc.shape
        kv_heads = k_loc.shape[1]
        piece_len = tok_dev // 2
        tiles = tok_dev // TILE
        rank = lax.axis_index('cx') * size_cy + lax.axis_index('cy')

        def gather(k_src, v_src, first_head, heads):
            k_part = k_src[:, first_head:first_head + heads].transpose(1, 0, 2)
            v_part = v_src[:, first_head:first_head + heads].reshape(tok_dev // head_dim, head_dim, heads, head_dim).transpose(2, 0, 3, 1)
            part = jnp.stack([k_part, v_part.reshape(heads, tok_dev, head_dim)])
            return lax.all_gather(part, ('cx', 'cy'))

        gathered = [gather(k_loc, v_loc, *CHUNKS[0])]
        below = jnp.sum(doc_loc[None, :] < jnp.arange(DOCS, dtype=jnp.int32)[:, None], axis=1, dtype=jnp.int32)
        below = lax.psum(below, ('cx', 'cy'))
        below, k_rest, v_rest = lax.optimization_barrier((below, k_loc, v_loc))
        gathered += [gather(k_rest, v_rest, *chunk) for chunk in CHUNKS[1:]]
        starts = jnp.zeros_like(doc_loc)
        for doc in range(DOCS):
            starts = jnp.where(doc_loc == doc, below[doc], starts)
        starts = starts.reshape(tiles, 1, TILE)
        tile_ids = jnp.arange(tiles, dtype=jnp.int32)
        half = tiles // 2
        tile_blk = jnp.where(tile_ids < half, rank * half + tile_ids, (2 * group - 1 - rank) * half + tile_ids - half).astype(jnp.int32)
        tab = jnp.stack([starts[:, 0, 0] // UNIT, tile_blk, starts[:, 0, TILE - 1]])
        first_lo = jnp.maximum(starts[0, 0, 0] - (BLK - UNIT), 0) // piece_len
        second_lo = jnp.maximum(starts[half, 0, 0] - (BLK - UNIT), 0) // piece_len
        first_end = rank + 1
        rng = jnp.stack([jnp.stack([jnp.minimum(first_lo, second_lo), first_end]), jnp.stack([jnp.maximum(second_lo, first_end), 2 * group - rank])]).astype(jnp.int32)

        out = None
        for (first_head, _), kv_all in zip(CHUNKS, gathered):
            out = attend(tab, rng, kv_all, q_loc, starts, out, first_head)
        return out

    return jax.shard_map(per_device, mesh=mesh, in_specs=(seq_spec, seq_spec, seq_spec, doc_spec), out_specs=seq_spec, check_vma=False)
```
